32 devices in a mesh: member: 2 (over x), gx: 16 (over z, y, core).
Axes of the slice: x: 2, y: 2, z: 4, core: 2. Of those that a mesh axis runs over, the one named last changes fastest.
Arguments:
- spectrum: float32 [36, 32, 256, 128], P(None, None, ('member', 'gx')), parts along dimension 2, may hold values from 0 to 1
- wind: float32 [2, 256, 128], P(None, ('member', 'gx')), parts along dimension 1, may hold values from -32 to 32
- land_sea: int32 [128, 128], P('gx'), may hold values 0 or 1
- band_rows: int32 [128], replicated, may hold values from 0 to 127, each once
Outputs:
- spectrum_next: float32 [36, 32, 256, 128], P(None, None, ('member', 'gx')), parts along dimension 2
- ocean_fields: float32 [4, 128, 256], P(None, 'gx', 'member'), parts along dimension 2
The draws below stay inside these ranges and needn't reach their ends.
There are 2 independent parts, one for each index of `member`. The reference program is written for one: setup_inputs(seed, part) draws one part's arguments, and reference() takes and returns one part's arrays. A program takes and returns all parts, laid end to end along the dimension named above; an argument that names none is the same for every part. Nothing has to cross between parts.
Inputs may be any that keep to these rules, and one draw needn't show every extreme that they name: band_rows names each of the 128 latitude rows exactly once.
All inputs are finite; a program needn't handle non-finite values. No bound on the sum of `land_sea` on one device may be relied on, other than what follows from the above.
Results may differ from the reference program's by a relative error of at most 0.00015.
Values sent between devices are 32-bit elements; how exact they have to be, the bound alone decides.
A program may use at most 128 MiB of HBM per device.

```python
import math
import jax
import jax.numpy as jnp
from jax import lax

DIRS = 36
FREQS = 32
LAT = 128
STEPS = 3
NLON = 128


def touch_ends(values, key, least, largest):
    index_at = [jax.random.randint(jax.random.fold_in(key, axis), (), 0, length) for axis, length in enumerate(values.shape)]
    longest = values.shape.index(max(values.shape))
    beside = index_at[:longest] + [(index_at[longest] + 1) % values.shape[longest]] + index_at[longest + 1:]
    return values.at[tuple(index_at)].set(least).at[tuple(beside)].set(largest)


def block_levels(own_key, shape, shards, least, largest):
    def one(position, shards_of):
        draws = jax.random.uniform(jax.random.fold_in(jax.random.fold_in(own_key, 6), position), (shards_of,), jnp.float32, least / len(shards), largest / len(shards))
        return jnp.repeat(jnp.exp(draws), shape[position] // shards_of).reshape((-1,) + (1,) * (len(shape) - position - 1))

    loudness = one(*shards[0])
    for cut in shards[1:]:
        loudness = loudness * one(*cut)
    return loudness


def centred(rng, dims, width, bound, cuts=(), kind=jnp.bfloat16):
    level = block_levels(rng, dims, cuts, -0.22, 0.18) if cuts else 1.0
    array = jax.random.normal(rng, dims, jnp.float32) * width * level
    return jnp.minimum(jnp.maximum(array, -bound), bound).astype(kind)


def setup_inputs(seed: int = 0, part: int = 0) -> dict:
    keys = jax.random.split(jax.random.key(seed), 5)
    part_keys = jax.random.split(jax.random.fold_in(keys[4], part), 5)
    spectrum = jnp.clip(1.0 * jax.random.uniform(part_keys[0], (DIRS, FREQS, NLON, LAT), jnp.float32) ** block_levels(part_keys[0], (DIRS, FREQS, NLON, LAT), ((2, 16),), -0.2, 0.2), 0.0, 1.0)
    wind = centred(part_keys[1], (2, NLON, LAT), 8.0, 32.0, ((1, 16),), jnp.float32)
    land_sea = touch_ends((jax.random.randint(keys[2], (NLON, LAT), 0, 4) < 3).astype(jnp.int32), jax.random.fold_in(keys[2], 1), 0, 1)
    band_rows = jax.random.permutation(keys[3], LAT).astype(jnp.int32)
    return dict(spectrum=spectrum, wind=wind, land_sea=land_sea, band_rows=band_rows)


def wave_tables(directions, frequencies):
    angles = (jnp.arange(directions, dtype=jnp.float32) + 0.5) * (2.0 * math.pi / directions)
    levels = jnp.arange(frequencies, dtype=jnp.float32)
    shrink = jnp.power(jnp.float32(1.1), -levels)
    frequency = 0.0418 / shrink
    inverse_speed = 2.0 * math.pi * frequency / 9.81
    weight = (levels + 1.0) / frequencies
    cosine_dir = jnp.cos(angles)[:, None]
    sine_dir = jnp.sin(angles)[:, None]
    courant_x = 0.45 * shrink[None, :] * cosine_dir
    courant_y = 0.45 * shrink[None, :] * sine_dir
    factor = 3.0 / math.sqrt(directions * frequencies)
    project = jnp.stack([factor * weight[None, :] * cosine_dir, factor * weight[None, :] * sine_dir])
    return (courant_x, courant_y, cosine_dir, sine_dir, inverse_speed, weight * weight, project)

def upwind(center, west_cell, east_cell, courant_x, courant_y):
    along_x = courant_x[:, :, None, None]
    along_y = courant_y[:, :, None, None]
    border = jnp.zeros_like(center[..., :1])
    south_cell = jnp.concatenate([border, center[..., :-1]], axis=3)
    north_cell = jnp.concatenate([center[..., 1:], border], axis=3)
    return center - jnp.maximum(along_x, 0.0) * (center - west_cell) + jnp.maximum(-along_x, 0.0) * (east_cell - center) - jnp.maximum(along_y, 0.0) * (center - south_cell) + jnp.maximum(-along_y, 0.0) * (north_cell - center)

def sources(advected, wind_east, wind_north, sea_mask, tables):
    cosine_dir, sine_dir, inverse_speed, weight_two = (tables[2], tables[3], tables[4], tables[5])
    advected = advected * sea_mask
    energy = lax.optimization_barrier(jnp.mean(advected, axis=(0, 1)))
    wind_ratio = (wind_east * cosine_dir[:, :, None, None] + wind_north * sine_dir[:, :, None, None]) * inverse_speed[None, :, None, None]
    growth = 0.05 * jnp.clip(wind_ratio - 1.0, 0.0, 4.0)
    damping = 0.3 * weight_two[None, :, None, None] * (energy / (0.5 + energy))
    return (advected * (1.0 + growth) / (1.0 + damping), growth * advected)

def coupling_fields(input_flux, current, project):
    stress = jnp.einsum('cij,ijxy->cxy', project, input_flux, precision=lax.Precision.HIGHEST)
    stokes = jnp.einsum('cij,ijxy->cxy', project, current, precision=lax.Precision.HIGHEST)
    return jnp.concatenate([stress, stokes], axis=0)

def reference(spectrum, wind, land_sea, band_rows):
    tables = wave_tables(spectrum.shape[0], spectrum.shape[1])
    sea_mask = land_sea.astype(jnp.float32)
    current = spectrum
    for step_index in range(STEPS):
        advected = upwind(current, jnp.roll(current, 1, axis=2), jnp.roll(current, -1, axis=2), tables[0], tables[1])
        current, input_flux = sources(advected, wind[0], wind[1], sea_mask, tables)
    fields = coupling_fields(input_flux, current, tables[6])
    ocean_fields = jnp.transpose(fields[:, :, band_rows], (0, 2, 1))
    return (current, ocean_fields)
```

```python
import functools
import math

import jax
import jax.numpy as jnp
import numpy as np
from jax import lax
from jax.experimental import pallas as pl
from jax.experimental.pallas import tpu as pltpu
from jax.sharding import PartitionSpec as P

STEPS = 3
SUB = 8
LEFT, RIGHT = 8, 10


def tables(directions, frequencies):
    angles = (np.arange(directions) + 0.5) * (2.0 * math.pi / directions)
    levels = np.arange(frequencies)
    shrink = 1.1 ** (-levels.astype(np.float64))
    inverse_speed = 2.0 * math.pi * (0.0418 / shrink) / 9.81
    weight = (levels + 1.0) / frequencies
    per_freq = np.stack([0.45 * shrink, inverse_speed, 0.3 * weight * weight,
                         weight * 3.0 / math.sqrt(directions * frequencies)])
    groups = frequencies // SUB
    per_freq = np.broadcast_to(per_freq.reshape(4, groups, SUB, 1), (4, groups, SUB, 128))
    return (np.stack([np.cos(angles), np.sin(angles)]).astype(np.float32),
            np.ascontiguousarray(per_freq).astype(np.float32))


def kernel(n, dirs, groups, trig, freq, spec, wind, land, bands, out, ocean,
           x_ref, w_ref, g_ref, send_e, send_w, halo_l, halo_r, wind_h, land_h,
           wind_b, mask_b, r_ref, e_send, e_halo, rows, sends, recv,
           in_sem, out_sem, ssem, rsem, a_ssem, a_rsem):
    me = lax.axis_index("gx")
    right, left = lax.rem(me + 1, n), lax.rem(me + n - 1, n)
    quarter = dirs // 4
    qrows = quarter * groups * SUB * SUB
    cells = dirs * groups * SUB
    lane = lax.broadcasted_iota(jnp.int32, (SUB, 128), 1)
    quads = [(q * quarter, q in (0, 3), q in (0, 1)) for q in range(4)]

    def in_copy(q):
        part = pl.ds(q * qrows, qrows)
        return pltpu.make_async_copy(spec.at[part], x_ref.at[part], in_sem.at[q])

    def out_copy(q):
        part = pl.ds(q * qrows, qrows)
        return pltpu.make_async_copy(x_ref.at[part], out.at[part], out_sem.at[q])

    for q in range(4):
        in_copy(q).start()

    barrier = pltpu.get_barrier_semaphore()

    def greet(i, _):
        pl.semaphore_signal(barrier, inc=1, device_id={"gx": lax.rem(me + i, n)},
                            device_id_type=pl.DeviceIdType.MESH)
        return 0

    lax.fori_loop(1, n, greet, 0)

    def remote(src, dst, slot, target):
        return pltpu.make_async_remote_copy(
            src_ref=src, dst_ref=dst, send_sem=ssem.at[slot], recv_sem=rsem.at[slot],
            device_id={"gx": target}, device_id_type=pl.DeviceIdType.MESH)

    bulk_e = [remote(send_e.at[k], halo_l.at[k], k, right) for k in range(3)]
    bulk_w = [remote(send_w.at[k], halo_r.at[k], 3 + k, left) for k in range(3)]
    small = [remote(wind, wind_h.at[0], 6, right), remote(wind, wind_h.at[1], 7, left),
             remote(land, land_h.at[0], 8, right), remote(land, land_h.at[1], 9, left)]
    energy_msg = [[remote(e_send.at[s], e_halo.at[s, 0], 10 + 2 * s, right),
                   remote(e_send.at[s], e_halo.at[s, 1], 11 + 2 * s, left)] for s in range(2)]

    for q, (d0, east, north) in enumerate(quads):
        in_copy(q).wait()
        base = d0 * groups
        local = (0 if q in (0, 1) else quarter) * groups

        def pack(i, _, base=base, local=local, east=east):
            for k in range(3):
                column = SUB - 1 - k if east else k
                value = x_ref[pl.ds((base + i) * SUB * SUB + column, SUB, stride=SUB), :]
                (send_e if east else send_w)[k, local + i] = value
            return 0

        lax.fori_loop(0, quarter * groups, pack, 0, unroll=4)

    def spread(slot, wind_tile, land_tile, column):
        for c in range(2):
            wind_b[c, slot] = jnp.broadcast_to(wind_tile[c][column:column + 1], (SUB, 128))
        mask_b[slot] = jnp.broadcast_to(
            land_tile[column:column + 1].astype(jnp.float32), (SUB, 128))

    own_wind = [wind[0], wind[1]]
    own_land = land[...]
    for x in range(SUB):
        spread(x, own_wind, own_land, x)

    pl.semaphore_wait(barrier, n - 1)
    for copy in small + [bulk_e[0], bulk_w[0], bulk_e[1], bulk_w[1]]:
        copy.start()

    def scalars(d):
        return trig[0, d], trig[1, d]

    def coefficients(cosine, sine, f, east, north):
        k = freq[0, f]
        along_x = k * (cosine if east else -cosine)
        along_y = k * (sine if north else -sine)
        centre = 1.0 - along_x - along_y
        return centre, along_x, jnp.where(lane == (0 if north else 127), 0.0, along_y)

    def shifted(value, north):
        return pltpu.roll(value, 1 if north else 127, 1)

    def growth_of(cosine, sine, f, slot):
        ratio = (wind_b[0, slot] * cosine + wind_b[1, slot] * sine) * freq[1, f]
        return 0.05 * jnp.minimum(jnp.maximum(ratio - 1.0, 0.0), 4.0)

    zero = jnp.zeros((SUB, 128), jnp.float32)

    def main(step, sums):
        for d0, east, north in quads:
            def body(i, sums, d0=d0, east=east, north=north):
                d = d0 + i
                cosine, sine = scalars(d)
                sums = list(sums)
                if step == 0:
                    speed = [wind_b[0, x] * cosine + wind_b[1, x] * sine for x in range(SUB)]
                for f in range(groups):
                    centre, along_x, along_y = coefficients(cosine, sine, f, east, north)
                    before = None
                    for x in (range(SUB) if east else range(SUB - 1, -1, -1)):
                        at = (d * groups + f) * SUB + x
                        if step == 0:
                            value = x_ref[pl.ds((d * groups + f) * SUB * SUB + x, SUB, stride=SUB), :]
                            g_ref[at] = 0.05 * jnp.minimum(
                                jnp.maximum(speed[x] * freq[1, f] - 1.0, 0.0), 4.0)
                        else:
                            value = w_ref[at] * (1.0 + g_ref[at]) * r_ref[x, f]
                        new = centre * value + along_y * shifted(value, north)
                        if before is not None:
                            new = new + along_x * before
                        before = value
                        w_ref[at] = new
                        sums[x] = sums[x] + new
                return tuple(sums)

            sums = lax.fori_loop(0, quarter, body, tuple(sums))
        return sums

    def fix(step, sums):
        first, last = sums[0], sums[SUB - 1]
        for q, (d0, east, north) in enumerate(quads):
            halo = halo_l if east else halo_r
            slot = LEFT if east else RIGHT
            edge = 0 if east else SUB - 1
            local = (0 if q in (0, 1) else quarter) * groups

            def body(i, total, d0=d0, east=east, north=north, halo=halo, slot=slot,
                     edge=edge, local=local):
                d = d0 + i
                cosine, sine = scalars(d)
                for f in range(groups):
                    centre, along_x, along_y = coefficients(cosine, sine, f, east, north)
                    at = local + i * groups + f

                    def advance(value, upwind, depth, s):
                        moved = centre * value + along_x * upwind + along_y * shifted(value, north)
                        growth = growth_of(cosine, sine, f, slot + depth)
                        return moved * (1.0 + growth) * r_ref[slot + depth + 4 * (s if depth == 0 else 0), f]

                    if step == 0:
                        flow = halo[0, at]
                    elif step == 1:
                        flow = advance(halo[0, at], halo[1, at], 0, 0)
                        halo[0, at] = flow
                    else:
                        far = advance(halo[1, at], halo[2, at], 1, 0)
                        flow = advance(halo[0, at], far, 0, 1)
                    extra = along_x * flow
                    cell = (d * groups + f) * SUB + edge
                    w_ref[cell] = w_ref[cell] + extra
                    total = total + extra
                return total

            if east:
                first = lax.fori_loop(0, quarter, body, first)
            else:
                last = lax.fori_loop(0, quarter, body, last)
        return (first,) + tuple(sums[1:-1]) + (last,)

    def energy_tile(sums):
        return jnp.concatenate(
            [jnp.sum(s * mask_b[x], axis=0, keepdims=True) for x, s in enumerate(sums)],
            axis=0) * (1.0 / cells)

    def factor(tile, column, mask_slot, slot):
        ratio = jnp.broadcast_to(tile[column:column + 1], (SUB, 128))
        for f in range(groups):
            r_ref[slot, f] = mask_b[mask_slot] / (1.0 + freq[2, f] * ratio)

    def own_factors(tile):
        ratio = tile / (0.5 + tile)
        for x in range(SUB):
            factor(ratio, x, x, x)

    sums = main(0, (zero,) * SUB)
    for copy in small:
        copy.wait()
    for side in range(2):
        tiles = [wind_h[side, 0], wind_h[side, 1]]
        land_tile = land_h[side]
        for depth in range(2):
            spread((LEFT if side == 0 else RIGHT) + depth, tiles, land_tile,
                   SUB - 1 - depth if side == 0 else depth)
    bulk_e[0].wait()
    bulk_w[0].wait()
    sums = fix(0, sums)
    for step in (1, 2):
        tile = energy_tile(sums)
        e_send[step - 1] = tile
        own_factors(tile)
        for copy in energy_msg[step - 1]:
            copy.start()
        if step == 1:
            bulk_e[2].start()
            bulk_w[2].start()
        sums = main(step, (zero,) * SUB)
        bulk_e[step].wait()
        bulk_w[step].wait()
        for copy in energy_msg[step - 1]:
            copy.wait()
        for side in range(2):
            seen = e_halo[step - 1, side]
            ratio = seen / (0.5 + seen)
            base = LEFT if side == 0 else RIGHT
            for depth in range(3 - step):
                factor(ratio, SUB - 1 - depth if side == 0 else depth, base + depth,
                       base + depth + 4 * (step - 1))
        sums = fix(step, sums)

    own_factors(energy_tile(sums))

    stress = [[zero] * SUB, [zero] * SUB]
    fields = [[None] * SUB for _ in range(4)]

    for q, (d0, east, north) in enumerate(quads):
        def body(i, carry, d0=d0):
            d = d0 + i
            cosine, sine = scalars(d)
            for x in range(SUB):
                flux, drift = zero, zero
                for f in range(groups):
                    at = (d * groups + f) * SUB + x
                    moved = w_ref[at]
                    flow = g_ref[at] * moved
                    after = (moved + flow) * r_ref[x, f]
                    x_ref[pl.ds((d * groups + f) * SUB * SUB + x, SUB, stride=SUB), :] = after
                    flux = flux + freq[3, f] * flow
                    drift = drift + freq[3, f] * after
                carry = list(carry)
                carry[x] = carry[x] + cosine * flux
                carry[SUB + x] = carry[SUB + x] + sine * flux
                carry[2 * SUB + x] = carry[2 * SUB + x] + cosine * drift
                carry[3 * SUB + x] = carry[3 * SUB + x] + sine * drift
            return tuple(carry)

        carry = lax.fori_loop(0, quarter, body, (zero,) * (4 * SUB) if q == 0 else carry)
        out_copy(q).start()

    total = []
    for j, value in enumerate(carry):
        if j < 2 * SUB:
            value = value * mask_b[j % SUB]
        total.append(jnp.sum(value, axis=0, keepdims=True))
    total.append(jnp.zeros((128 - 4 * SUB, 128), jnp.float32))
    stacked = jnp.concatenate(total, axis=0)
    lat = lax.broadcasted_iota(jnp.int32, (128, 128), 0)
    pick = (lat == bands[...]).astype(jnp.float32)
    picked = jnp.dot(stacked, pick, precision=lax.Precision.HIGHEST,
                     preferred_element_type=jnp.float32)
    rows[...] = picked.T
    band = 128 // n
    for k in range(n):
        sends[k] = rows[pl.ds(k * band, band), :]

    def exchange(i):
        target = lax.rem(me + i, n)
        return pltpu.make_async_remote_copy(
            src_ref=sends.at[target], dst_ref=recv.at[me], send_sem=a_ssem.at[i],
            recv_sem=a_rsem.at[i], device_id={"gx": target},
            device_id_type=pl.DeviceIdType.MESH)

    def begin(i, _):
        exchange(i).start()
        return 0

    def finish(i, _):
        exchange(i).wait()
        return 0

    lax.fori_loop(1, n, begin, 0)
    recv[pl.ds(me, 1)] = sends[pl.ds(me, 1)]
    lax.fori_loop(1, n, finish, 0)
    per_tile = 128 // SUB
    block = lax.broadcasted_iota(jnp.int32, (band, 128), 1) // SUB
    for tile in range(max(1, n // per_tile)):
        for c in range(4):
            built = jnp.zeros((band, 128), jnp.float32)
            for k in range(min(n, per_tile)):
                moved = pltpu.roll(recv[tile * per_tile + k], (SUB * (k - c)) % 128, 1)
                built = jnp.where(block == k, moved, built)
            ocean[c, :, tile * 128:(tile + 1) * 128] = built
    for q in range(4):
        out_copy(q).wait()


def per_device(n, spectrum, wind, land_sea, band_rows):
    dirs, freqs, columns, lats = spectrum.shape
    groups = freqs // SUB
    trig, freq = tables(dirs, freqs)
    half = dirs // 2 * groups
    band = lats // n
    f32 = jnp.float32
    vmem = pl.BlockSpec(memory_space=pltpu.VMEM)
    anywhere = pl.BlockSpec(memory_space=pl.ANY)
    cells = dirs * groups * SUB
    after, ocean = pl.pallas_call(
        functools.partial(kernel, n, dirs, groups),
        out_shape=(jax.ShapeDtypeStruct((cells * SUB, lats), f32),
                   jax.ShapeDtypeStruct((4, band, columns * n), f32)),
        in_specs=[pl.BlockSpec(memory_space=pltpu.SMEM), vmem, anywhere, vmem, vmem, vmem],
        out_specs=(anywhere, vmem),
        scratch_shapes=[
            pltpu.VMEM((cells * SUB, lats), f32),
            pltpu.VMEM((cells, SUB, lats), f32),
            pltpu.VMEM((cells, SUB, lats), f32),
            pltpu.VMEM((3, half, SUB, lats), f32),
            pltpu.VMEM((3, half, SUB, lats), f32),
            pltpu.VMEM((3, half, SUB, lats), f32),
            pltpu.VMEM((3, half, SUB, lats), f32),
            pltpu.VMEM((2, 2, SUB, lats), f32),
            pltpu.VMEM((2, SUB, lats), jnp.int32),
            pltpu.VMEM((2, 12, SUB, lats), f32),
            pltpu.VMEM((12, SUB, lats), f32),
            pltpu.VMEM((16, groups, SUB, lats), f32),
            pltpu.VMEM((2, SUB, lats), f32),
            pltpu.VMEM((2, 2, SUB, lats), f32),
            pltpu.VMEM((128, 128), f32),
            pltpu.VMEM((n, band, 128), f32),
            pltpu.VMEM((n, band, 128), f32),
            pltpu.SemaphoreType.DMA((4,)),
            pltpu.SemaphoreType.DMA((4,)),
            pltpu.SemaphoreType.DMA((14,)),
            pltpu.SemaphoreType.DMA((14,)),
            pltpu.SemaphoreType.DMA((n,)),
            pltpu.SemaphoreType.DMA((n,)),
        ],
        compiler_params=pltpu.CompilerParams(
            collective_id=0, has_side_effects=True, vmem_limit_bytes=48 * 2**20),
        name="wave_window",
    )(jnp.asarray(trig), jnp.asarray(freq), spectrum.reshape(cells * SUB, lats), wind, land_sea,
      band_rows.reshape(1, lats))
    return after.reshape(spectrum.shape), ocean


def solution(mesh):
    placed = (
        P(None, None, ("member", "gx"), None),
        P(None, ("member", "gx"), None),
        P("gx", None),
        P(),
    )
    return jax.shard_map(
        functools.partial(per_device, mesh.shape["gx"]),
        mesh=mesh,
        in_specs=placed,
        out_specs=(P(None, None, ("member", "gx"), None), P(None, "gx", "member")),
        check_vma=False,
    )
```

```python
import functools
import math

import jax
import jax.numpy as jnp
import numpy as np
from jax import lax
from jax.experimental import pallas as pl
from jax.experimental.pallas import tpu as pltpu
from jax.sharding import PartitionSpec as P

STEPS = 3
SUB = 8
LEFT, RIGHT = 8, 10


def tables(directions, frequencies):
    angles = (np.arange(directions) + 0.5) * (2.0 * math.pi / directions)
    levels = np.arange(frequencies)
    shrink = 1.1 ** (-levels.astype(np.float64))
    inverse_speed = 2.0 * math.pi * (0.0418 / shrink) / 9.81
    weight = (levels + 1.0) / frequencies
    per_freq = np.stack([0.45 * shrink, inverse_speed, 0.3 * weight * weight,
                         weight * 3.0 / math.sqrt(directions * frequencies)])
    groups = frequencies // SUB
    per_freq = np.broadcast_to(per_freq.reshape(4, groups, SUB, 1), (4, groups, SUB, 128))
    return (np.stack([np.cos(angles), np.sin(angles)]).astype(np.float32),
            np.ascontiguousarray(per_freq).astype(np.float32))


def kernel(n, dirs, groups, trig_in, freq_in, spec, wind_in, land_in, bands_in, out, ocean,
           trig, freq, wind, land, bands, x_ref, w_ref, g_ref, send_e, send_w, halo_l, halo_r, wind_h, land_h,
           wind_b, mask_b, r_ref, drift_ref, e_send, e_halo, rows, sends, recv,
           in_sem, small_sem, ssem, rsem, a_ssem, a_rsem):
    me = lax.axis_index("gx")
    right, left = lax.rem(me + 1, n), lax.rem(me + n - 1, n)
    quarter = dirs // 4
    qrows = quarter * groups * SUB * SUB
    cells = dirs * groups * SUB
    lane = lax.broadcasted_iota(jnp.int32, (SUB, 128), 1)
    quads = [(q * quarter, q in (0, 3), q in (0, 1)) for q in range(4)]

    def in_copy(q):
        part = pl.ds(q * qrows, qrows)
        return pltpu.make_async_copy(spec.at[part], x_ref.at[part], in_sem.at[q])

    tables_in = [pltpu.make_async_copy(src, dst, small_sem.at[i]) for i, (src, dst) in enumerate(
        [(trig_in, trig), (freq_in, freq), (wind_in, wind), (land_in, land), (bands_in, bands)])]
    for copy in tables_in:
        copy.start()
    for q in range(4):
        in_copy(q).start()

    barrier = pltpu.get_barrier_semaphore()

    def greet(i, _):
        pl.semaphore_signal(barrier, inc=1, device_id={"gx": lax.rem(me + i, n)},
                            device_id_type=pl.DeviceIdType.MESH)
        return 0

    lax.fori_loop(1, n, greet, 0)

    def remote(src, dst, slot, target):
        return pltpu.make_async_remote_copy(
            src_ref=src, dst_ref=dst, send_sem=ssem.at[slot], recv_sem=rsem.at[slot],
            device_id={"gx": target}, device_id_type=pl.DeviceIdType.MESH)

    bulk_e = [remote(send_e.at[k], halo_l.at[k], k, right) for k in range(3)]
    bulk_w = [remote(send_w.at[k], halo_r.at[k], 3 + k, left) for k in range(3)]
    small = [remote(wind, wind_h.at[0], 6, right), remote(wind, wind_h.at[1], 7, left),
             remote(land, land_h.at[0], 8, right), remote(land, land_h.at[1], 9, left)]
    energy_msg = [[remote(e_send.at[s], e_halo.at[s, 0], 10 + 2 * s, right),
                   remote(e_send.at[s], e_halo.at[s, 1], 11 + 2 * s, left)] for s in range(2)]

    for q, (d0, east, north) in enumerate(quads):
        in_copy(q).wait()
        base = d0 * groups
        local = (0 if q in (0, 1) else quarter) * groups

        def pack(i, _, base=base, local=local, east=east):
            for k in range(3):
                column = SUB - 1 - k if east else k
                value = x_ref[pl.ds((base + i) * SUB * SUB + column, SUB, stride=SUB), :]
                (send_e if east else send_w)[k, local + i] = value
            return 0

        lax.fori_loop(0, quarter * groups, pack, 0, unroll=4)

    for copy in tables_in:
        copy.wait()

    def spread(slot, wind_tile, land_tile, column):
        for c in range(2):
            wind_b[c, slot] = jnp.broadcast_to(wind_tile[c][column:column + 1], (SUB, 128))
        mask_b[slot] = jnp.broadcast_to(
            land_tile[column:column + 1].astype(jnp.float32), (SUB, 128))

    own_wind = [wind[0], wind[1]]
    own_land = land[...]
    for x in range(SUB):
        spread(x, own_wind, own_land, x)

    pl.semaphore_wait(barrier, n - 1)
    for copy in small + [bulk_e[0], bulk_w[0], bulk_e[1], bulk_w[1]]:
        copy.start()

    def scalars(d):
        return trig[0, d], trig[1, d]

    def coefficients(cosine, sine, f, east, north):
        k = freq[0, f]
        along_x = k * (cosine if east else -cosine)
        along_y = k * (sine if north else -sine)
        centre = 1.0 - along_x - along_y
        return centre, along_x, jnp.where(lane == (0 if north else 127), 0.0, along_y)

    def shifted(value, north):
        return pltpu.roll(value, 1 if north else 127, 1)

    def growth_of(cosine, sine, f, slot):
        ratio = (wind_b[0, slot] * cosine + wind_b[1, slot] * sine) * freq[1, f]
        return 0.05 * jnp.minimum(jnp.maximum(ratio - 1.0, 0.0), 4.0)

    zero = jnp.zeros((SUB, 128), jnp.float32)

    def main(step, sums):
        for d0, east, north in quads:
            def body(i, sums, d0=d0, east=east, north=north):
                d = d0 + i
                cosine, sine = scalars(d)
                sums = list(sums)
                if step == 0:
                    speed = [wind_b[0, x] * cosine + wind_b[1, x] * sine for x in range(SUB)]
                for f in range(groups):
                    centre, along_x, along_y = coefficients(cosine, sine, f, east, north)
                    before = None
                    for x in (range(SUB) if east else range(SUB - 1, -1, -1)):
                        at = (d * groups + f) * SUB + x
                        if step == 0:
                            value = x_ref[pl.ds((d * groups + f) * SUB * SUB + x, SUB, stride=SUB), :]
                            g_ref[at] = 0.05 * jnp.minimum(
                                jnp.maximum(speed[x] * freq[1, f] - 1.0, 0.0), 4.0)
                        else:
                            value = w_ref[at] * (1.0 + g_ref[at]) * r_ref[x, f]
                        new = centre * value + along_y * shifted(value, north)
                        if before is not None:
                            new = new + along_x * before
                        before = value
                        w_ref[at] = new
                        sums[x] = sums[x] + new
                return tuple(sums)

            sums = lax.fori_loop(0, quarter, body, tuple(sums))
        return sums

    def fix(step, sums):
        first, last = sums[0], sums[SUB - 1]
        for q, (d0, east, north) in enumerate(quads):
            halo = halo_l if east else halo_r
            slot = LEFT if east else RIGHT
            edge = 0 if east else SUB - 1
            local = (0 if q in (0, 1) else quarter) * groups

            def body(i, total, d0=d0, east=east, north=north, halo=halo, slot=slot,
                     edge=edge, local=local):
                d = d0 + i
                cosine, sine = scalars(d)
                for f in range(groups):
                    centre, along_x, along_y = coefficients(cosine, sine, f, east, north)
                    at = local + i * groups + f

                    def advance(value, upwind, depth, s):
                        moved = centre * value + along_x * upwind + along_y * shifted(value, north)
                        growth = growth_of(cosine, sine, f, slot + depth)
                        return moved * (1.0 + growth) * r_ref[slot + depth + 4 * (s if depth == 0 else 0), f]

                    if step == 0:
                        flow = halo[0, at]
                    elif step == 1:
                        flow = advance(halo[0, at], halo[1, at], 0, 0)
                        halo[0, at] = flow
                    else:
                        far = advance(halo[1, at], halo[2, at], 1, 0)
                        flow = advance(halo[0, at], far, 0, 1)
                    extra = along_x * flow
                    cell = (d * groups + f) * SUB + edge
                    w_ref[cell] = w_ref[cell] + extra
                    total = total + extra
                return total

            if east:
                first = lax.fori_loop(0, quarter, body, first)
            else:
                last = lax.fori_loop(0, quarter, body, last)
        return (first,) + tuple(sums[1:-1]) + (last,)

    def energy_tile(sums):
        return jnp.concatenate(
            [jnp.sum(s * mask_b[x], axis=0, keepdims=True) for x, s in enumerate(sums)],
            axis=0) * (1.0 / cells)

    def factor(tile, column, mask_slot, slot):
        ratio = jnp.broadcast_to(tile[column:column + 1], (SUB, 128))
        for f in range(groups):
            r_ref[slot, f] = mask_b[mask_slot] / (1.0 + freq[2, f] * ratio)

    def own_factors(tile):
        ratio = tile / (0.5 + tile)
        for x in range(SUB):
            factor(ratio, x, x, x)

    sums = main(0, (zero,) * SUB)
    for copy in small:
        copy.wait()
    for side in range(2):
        tiles = [wind_h[side, 0], wind_h[side, 1]]
        land_tile = land_h[side]
        for depth in range(2):
            spread((LEFT if side == 0 else RIGHT) + depth, tiles, land_tile,
                   SUB - 1 - depth if side == 0 else depth)
    bulk_e[0].wait()
    bulk_w[0].wait()
    sums = fix(0, sums)
    for step in (1, 2):
        tile = energy_tile(sums)
        e_send[step - 1] = tile
        own_factors(tile)
        for copy in energy_msg[step - 1]:
            copy.start()
        if step == 1:
            bulk_e[2].start()
            bulk_w[2].start()
        sums = main(step, (zero,) * SUB)
        bulk_e[step].wait()
        bulk_w[step].wait()
        for copy in energy_msg[step - 1]:
            copy.wait()
        for side in range(2):
            seen = e_halo[step - 1, side]
            ratio = seen / (0.5 + seen)
            base = LEFT if side == 0 else RIGHT
            for depth in range(3 - step):
                factor(ratio, SUB - 1 - depth if side == 0 else depth, base + depth,
                       base + depth + 4 * (step - 1))
        sums = fix(step, sums)

    own_factors(energy_tile(sums))

    def gather(d, carry):
        cosine, sine = scalars(d)
        carry = list(carry)
        for x in range(SUB):
            flux, drift = zero, zero
            for f in range(groups):
                at = (d * groups + f) * SUB + x
                moved = w_ref[at]
                flow = g_ref[at] * moved
                flux = flux + freq[3, f] * flow
                drift = drift + drift_ref[x, f] * (moved + flow)
            carry[x] = carry[x] + cosine * flux
            carry[SUB + x] = carry[SUB + x] + sine * flux
            carry[2 * SUB + x] = carry[2 * SUB + x] + cosine * drift
            carry[3 * SUB + x] = carry[3 * SUB + x] + sine * drift
        return tuple(carry)

    for x in range(SUB):
        for f in range(groups):
            drift_ref[x, f] = freq[3, f] * r_ref[x, f]
    carry = lax.fori_loop(0, dirs, gather, (zero,) * (4 * SUB))

    total = []
    for j, value in enumerate(carry):
        if j < 2 * SUB:
            value = value * mask_b[j % SUB]
        total.append(jnp.sum(value, axis=0, keepdims=True))
    total.append(jnp.zeros((128 - 4 * SUB, 128), jnp.float32))
    stacked = jnp.concatenate(total, axis=0)
    lat = lax.broadcasted_iota(jnp.int32, (128, 128), 0)
    pick = (lat == bands[...]).astype(jnp.float32)
    picked = jnp.dot(stacked, pick, precision=lax.Precision.HIGHEST,
                     preferred_element_type=jnp.float32)
    rows[...] = picked.T
    band = 128 // n
    for k in range(n):
        sends[k] = rows[pl.ds(k * band, band), :]

    def exchange(i):
        target = lax.rem(me + i, n)
        return pltpu.make_async_remote_copy(
            src_ref=sends.at[target], dst_ref=recv.at[me], send_sem=a_ssem.at[i],
            recv_sem=a_rsem.at[i], device_id={"gx": target},
            device_id_type=pl.DeviceIdType.MESH)

    def begin(i, _):
        exchange(i).start()
        return 0

    def finish(i, _):
        exchange(i).wait()
        return 0

    lax.fori_loop(1, n, begin, 0)
    recv[pl.ds(me, 1)] = sends[pl.ds(me, 1)]

    def write(d, _):
        for f in range(groups):
            for x in range(SUB):
                at = (d * groups + f) * SUB + x
                moved = w_ref[at]
                out[pl.ds((d * groups + f) * SUB * SUB + x, SUB, stride=SUB), :] = (
                    moved * (1.0 + g_ref[at]) * r_ref[x, f])
        return 0

    lax.fori_loop(0, dirs, write, 0)
    lax.fori_loop(1, n, finish, 0)
    per_tile = 128 // SUB
    block = lax.broadcasted_iota(jnp.int32, (band, 128), 1) // SUB
    for tile in range(max(1, n // per_tile)):
        for c in range(4):
            built = jnp.zeros((band, 128), jnp.float32)
            for k in range(min(n, per_tile)):
                moved = pltpu.roll(recv[tile * per_tile + k], (SUB * (k - c)) % 128, 1)
                built = jnp.where(block == k, moved, built)
            ocean[c, :, tile * 128:(tile + 1) * 128] = built


def per_device(n, spectrum, wind, land_sea, band_rows):
    dirs, freqs, columns, lats = spectrum.shape
    groups = freqs // SUB
    trig, freq = tables(dirs, freqs)
    half = dirs // 2 * groups
    band = lats // n
    f32 = jnp.float32
    vmem = pl.BlockSpec(memory_space=pltpu.VMEM)
    anywhere = pl.BlockSpec(memory_space=pltpu.HBM)
    cells = dirs * groups * SUB
    after, ocean = pl.pallas_call(
        functools.partial(kernel, n, dirs, groups),
        out_shape=(jax.ShapeDtypeStruct((cells * SUB, lats), f32),
                   jax.ShapeDtypeStruct((4, band, columns * n), f32)),
        in_specs=[anywhere] * 6,
        out_specs=(vmem, vmem),
        scratch_shapes=[
            pltpu.SMEM(trig.shape, f32),
            pltpu.VMEM(freq.shape, f32),
            pltpu.VMEM((2, SUB, lats), f32),
            pltpu.VMEM((SUB, lats), jnp.int32),
            pltpu.VMEM((1, lats), jnp.int32),
            pltpu.VMEM((cells * SUB, lats), f32),
            pltpu.VMEM((cells, SUB, lats), f32),
            pltpu.VMEM((cells, SUB, lats), f32),
            pltpu.VMEM((3, half, SUB, lats), f32),
            pltpu.VMEM((3, half, SUB, lats), f32),
            pltpu.VMEM((3, half, SUB, lats), f32),
            pltpu.VMEM((3, half, SUB, lats), f32),
            pltpu.VMEM((2, 2, SUB, lats), f32),
            pltpu.VMEM((2, SUB, lats), jnp.int32),
            pltpu.VMEM((2, 12, SUB, lats), f32),
            pltpu.VMEM((12, SUB, lats), f32),
            pltpu.VMEM((16, groups, SUB, lats), f32),
            pltpu.VMEM((SUB, groups, SUB, lats), f32),
            pltpu.VMEM((2, SUB, lats), f32),
            pltpu.VMEM((2, 2, SUB, lats), f32),
            pltpu.VMEM((128, 128), f32),
            pltpu.VMEM((n, band, 128), f32),
            pltpu.VMEM((n, band, 128), f32),
            pltpu.SemaphoreType.DMA((4,)),
            pltpu.SemaphoreType.DMA((5,)),
            pltpu.SemaphoreType.DMA((14,)),
            pltpu.SemaphoreType.DMA((14,)),
            pltpu.SemaphoreType.DMA((n,)),
            pltpu.SemaphoreType.DMA((n,)),
        ],
        compiler_params=pltpu.CompilerParams(
            collective_id=0, has_side_effects=True, vmem_limit_bytes=48 * 2**20),
        name="wave_window",
    )(jnp.asarray(trig), jnp.asarray(freq), spectrum.reshape(cells * SUB, lats), wind, land_sea,
      band_rows.reshape(1, lats))
    return after.reshape(spectrum.shape), ocean


def solution(mesh):
    placed = (
        P(None, None, ("member", "gx"), None),
        P(None, ("member", "gx"), None),
        P("gx", None),
        P(),
    )
    return jax.shard_map(
        functools.partial(per_device, mesh.shape["gx"]),
        mesh=mesh,
        in_specs=placed,
        out_specs=(P(None, None, ("member", "gx"), None), P(None, "gx", "member")),
        check_vma=False,
    )
```

```python
import functools
import math

import jax
import jax.numpy as jnp
from jax import lax
from jax.experimental import pallas as pl
from jax.experimental.pallas import tpu as pltpu
from jax.sharding import PartitionSpec as P

STEPS = 3
SUB = 8
LEFT, RIGHT = 8, 10


def kernel(n, dirs, groups, spec, wind_in, land_in, bands_in, out, ocean,
           trig, freq, wind, land, bands, x_ref, w_ref, g_ref, send_e, send_w, halo_l, halo_r, wind_h, land_h,
           wind_b, mask_b, r_ref, drift_ref, e_send, e_halo, rows, sends, recv,
           in_sem, small_sem, ssem, rsem, a_ssem, a_rsem):
    me = lax.axis_index("gx")
    right, left = lax.rem(me + 1, n), lax.rem(me + n - 1, n)
    quarter = dirs // 4
    qrows = quarter * groups * SUB * SUB
    cells = dirs * groups * SUB
    lane = lax.broadcasted_iota(jnp.int32, (SUB, 128), 1)
    quads = [(q * quarter, q in (0, 3), q in (0, 1)) for q in range(4)]

    def in_copy(q):
        part = pl.ds(q * qrows, qrows)
        return pltpu.make_async_copy(spec.at[part], x_ref.at[part], in_sem.at[q])

    tables_in = [pltpu.make_async_copy(src, dst, small_sem.at[i]) for i, (src, dst) in enumerate(
        [(wind_in, wind), (land_in, land), (bands_in, bands)])]
    for copy in tables_in:
        copy.start()
    for q in range(4):
        in_copy(q).start()

    for d in range(dirs):
        angle = (d + 0.5) * (2.0 * math.pi / dirs)
        trig[0, d] = jnp.float32(math.cos(angle))
        trig[1, d] = jnp.float32(math.sin(angle))
    freqs = groups * SUB
    for f in range(groups):
        level = (lax.broadcasted_iota(jnp.int32, (SUB, 128), 0) + f * SUB).astype(jnp.float32)
        weight = (level + 1.0) * (1.0 / freqs)
        grown = jnp.exp(level * math.log(1.1))
        freq[0, f] = 0.45 / grown
        freq[1, f] = grown * (2.0 * math.pi * 0.0418 / 9.81)
        freq[2, f] = 0.3 * weight * weight
        freq[3, f] = weight * (3.0 / math.sqrt(dirs * freqs))

    barrier = pltpu.get_barrier_semaphore()

    def greet(i, _):
        pl.semaphore_signal(barrier, inc=1, device_id={"gx": lax.rem(me + i, n)},
                            device_id_type=pl.DeviceIdType.MESH)
        return 0

    lax.fori_loop(1, n, greet, 0)

    def remote(src, dst, slot, target):
        return pltpu.make_async_remote_copy(
            src_ref=src, dst_ref=dst, send_sem=ssem.at[slot], recv_sem=rsem.at[slot],
            device_id={"gx": target}, device_id_type=pl.DeviceIdType.MESH)

    bulk_e = [remote(send_e.at[k], halo_l.at[k], k, right) for k in range(3)]
    bulk_w = [remote(send_w.at[k], halo_r.at[k], 3 + k, left) for k in range(3)]
    small = [remote(wind, wind_h.at[0], 6, right), remote(wind, wind_h.at[1], 7, left),
             remote(land, land_h.at[0], 8, right), remote(land, land_h.at[1], 9, left)]
    energy_msg = [[remote(e_send.at[s], e_halo.at[s, 0], 10 + 2 * s, right),
                   remote(e_send.at[s], e_halo.at[s, 1], 11 + 2 * s, left)] for s in range(2)]

    for q, (d0, east, north) in enumerate(quads):
        in_copy(q).wait()
        base = d0 * groups
        local = (0 if q in (0, 1) else quarter) * groups

        def pack(i, _, base=base, local=local, east=east):
            for k in range(3):
                column = SUB - 1 - k if east else k
                value = x_ref[pl.ds((base + i) * SUB * SUB + column, SUB, stride=SUB), :]
                (send_e if east else send_w)[k, local + i] = value
            return 0

        lax.fori_loop(0, quarter * groups, pack, 0, unroll=4)

    for copy in tables_in:
        copy.wait()

    def spread(slot, wind_tile, land_tile, column):
        for c in range(2):
            wind_b[c, slot] = jnp.broadcast_to(wind_tile[c][column:column + 1], (SUB, 128))
        mask_b[slot] = jnp.broadcast_to(
            land_tile[column:column + 1].astype(jnp.float32), (SUB, 128))

    own_wind = [wind[0], wind[1]]
    own_land = land[...]
    for x in range(SUB):
        spread(x, own_wind, own_land, x)

    pl.semaphore_wait(barrier, n - 1)
    for copy in small + [bulk_e[0], bulk_w[0], bulk_e[1], bulk_w[1]]:
        copy.start()

    def scalars(d):
        return trig[0, d], trig[1, d]

    halves = [(0, 2 * quarter, True), (quarter, 0, False)]

    def coefficients(cosine, sine, f, east, turn):
        k = freq[0, f]
        along_x = k * (cosine if east else -cosine)
        along_y = k * jnp.abs(sine)
        centre = 1.0 - along_x - along_y
        return centre, along_x, jnp.where(lane == 127 * turn, 0.0, along_y)

    def shifted(value, turn):
        return pltpu.roll(value, 1 + 126 * turn, 1)

    def growth_of(cosine, sine, f, slot):
        ratio = (wind_b[0, slot] * cosine + wind_b[1, slot] * sine) * freq[1, f]
        return 0.05 * jnp.minimum(jnp.maximum(ratio - 1.0, 0.0), 4.0)

    zero = jnp.zeros((SUB, 128), jnp.float32)

    def main(step, sums):
        for d0, skip, east in halves:
            def body(i, sums, d0=d0, skip=skip, east=east):
                turn = i // quarter
                d = d0 + i + skip * turn
                cosine, sine = scalars(d)
                sums = list(sums)
                if step == 0:
                    speed = [wind_b[0, x] * cosine + wind_b[1, x] * sine for x in range(SUB)]
                for f in range(groups):
                    centre, along_x, along_y = coefficients(cosine, sine, f, east, turn)
                    before = None
                    for x in (range(SUB) if east else range(SUB - 1, -1, -1)):
                        at = (d * groups + f) * SUB + x
                        if step == 0:
                            value = x_ref[pl.ds((d * groups + f) * SUB * SUB + x, SUB, stride=SUB), :]
                            g_ref[at] = 0.05 * jnp.minimum(
                                jnp.maximum(speed[x] * freq[1, f] - 1.0, 0.0), 4.0)
                        else:
                            value = w_ref[at] * (1.0 + g_ref[at]) * r_ref[x, f]
                        new = centre * value + along_y * shifted(value, turn)
                        if before is not None:
                            new = new + along_x * before
                        before = value
                        w_ref[at] = new
                        sums[x] = sums[x] + new
                return tuple(sums)

            sums = lax.fori_loop(0, 2 * quarter, body, tuple(sums))
        return sums

    def fix(step, sums):
        first, last = sums[0], sums[SUB - 1]
        for d0, skip, east in halves:
            halo = halo_l if east else halo_r
            slot = LEFT if east else RIGHT
            edge = 0 if east else SUB - 1

            def body(i, total, d0=d0, skip=skip, east=east, halo=halo, slot=slot, edge=edge):
                turn = i // quarter
                d = d0 + i + skip * turn
                cosine, sine = scalars(d)
                for f in range(groups):
                    centre, along_x, along_y = coefficients(cosine, sine, f, east, turn)
                    at = i * groups + f

                    def advance(value, upwind, depth, s):
                        moved = centre * value + along_x * upwind + along_y * shifted(value, turn)
                        growth = growth_of(cosine, sine, f, slot + depth)
                        return moved * (1.0 + growth) * r_ref[slot + depth + 4 * (s if depth == 0 else 0), f]

                    if step == 0:
                        flow = halo[0, at]
                    elif step == 1:
                        flow = advance(halo[0, at], halo[1, at], 0, 0)
                        halo[0, at] = flow
                    else:
                        far = advance(halo[1, at], halo[2, at], 1, 0)
                        flow = advance(halo[0, at], far, 0, 1)
                    extra = along_x * flow
                    cell = (d * groups + f) * SUB + edge
                    w_ref[cell] = w_ref[cell] + extra
                    total = total + extra
                return total

            if east:
                first = lax.fori_loop(0, 2 * quarter, body, first)
            else:
                last = lax.fori_loop(0, 2 * quarter, body, last)
        return (first,) + tuple(sums[1:-1]) + (last,)

    def energy_tile(sums):
        return jnp.concatenate(
            [jnp.sum(s * mask_b[x], axis=0, keepdims=True) for x, s in enumerate(sums)],
            axis=0) * (1.0 / cells)

    def factor(tile, column, mask_slot, slot):
        ratio = jnp.broadcast_to(tile[column:column + 1], (SUB, 128))
        for f in range(groups):
            r_ref[slot, f] = mask_b[mask_slot] / (1.0 + freq[2, f] * ratio)

    def own_factors(tile):
        ratio = tile / (0.5 + tile)
        for x in range(SUB):
            factor(ratio, x, x, x)

    sums = main(0, (zero,) * SUB)
    for copy in small:
        copy.wait()
    for side in range(2):
        tiles = [wind_h[side, 0], wind_h[side, 1]]
        land_tile = land_h[side]
        for depth in range(2):
            spread((LEFT if side == 0 else RIGHT) + depth, tiles, land_tile,
                   SUB - 1 - depth if side == 0 else depth)
    bulk_e[0].wait()
    bulk_w[0].wait()
    sums = fix(0, sums)
    for step in (1, 2):
        tile = energy_tile(sums)
        e_send[step - 1] = tile
        own_factors(tile)
        for copy in energy_msg[step - 1]:
            copy.start()
        if step == 1:
            bulk_e[2].start()
            bulk_w[2].start()
        sums = main(step, (zero,) * SUB)
        bulk_e[step].wait()
        bulk_w[step].wait()
        for copy in energy_msg[step - 1]:
            copy.wait()
        for side in range(2):
            seen = e_halo[step - 1, side]
            ratio = seen / (0.5 + seen)
            base = LEFT if side == 0 else RIGHT
            for depth in range(3 - step):
                factor(ratio, SUB - 1 - depth if side == 0 else depth, base + depth,
                       base + depth + 4 * (step - 1))
        sums = fix(step, sums)

    own_factors(energy_tile(sums))

    def gather(d, carry):
        cosine, sine = scalars(d)
        carry = list(carry)
        for x in range(SUB):
            flux, drift = zero, zero
            for f in range(groups):
                at = (d * groups + f) * SUB + x
                moved = w_ref[at]
                flow = g_ref[at] * moved
                flux = flux + freq[3, f] * flow
                drift = drift + drift_ref[x, f] * (moved + flow)
            carry[x] = carry[x] + cosine * flux
            carry[SUB + x] = carry[SUB + x] + sine * flux
            carry[2 * SUB + x] = carry[2 * SUB + x] + cosine * drift
            carry[3 * SUB + x] = carry[3 * SUB + x] + sine * drift
        return tuple(carry)

    for x in range(SUB):
        for f in range(groups):
            drift_ref[x, f] = freq[3, f] * r_ref[x, f]
    carry = lax.fori_loop(0, dirs, gather, (zero,) * (4 * SUB))

    total = []
    for j, value in enumerate(carry):
        if j < 2 * SUB:
            value = value * mask_b[j % SUB]
        total.append(jnp.sum(value, axis=0, keepdims=True))
    total.append(jnp.zeros((128 - 4 * SUB, 128), jnp.float32))
    stacked = jnp.concatenate(total, axis=0)
    lat = lax.broadcasted_iota(jnp.int32, (128, 128), 0)
    pick = (lat == bands[...]).astype(jnp.float32)
    picked = jnp.dot(stacked, pick, precision=lax.Precision.HIGHEST,
                     preferred_element_type=jnp.float32)
    rows[...] = picked.T
    band = 128 // n
    for k in range(n):
        sends[k] = rows[pl.ds(k * band, band), :]

    def exchange(i):
        target = lax.rem(me + i, n)
        return pltpu.make_async_remote_copy(
            src_ref=sends.at[target], dst_ref=recv.at[me], send_sem=a_ssem.at[i],
            recv_sem=a_rsem.at[i], device_id={"gx": target},
            device_id_type=pl.DeviceIdType.MESH)

    def begin(i, _):
        exchange(i).start()
        return 0

    def finish(i, _):
        exchange(i).wait()
        return 0

    lax.fori_loop(1, n, begin, 0)
    recv[pl.ds(me, 1)] = sends[pl.ds(me, 1)]

    def write(d, _):
        for f in range(groups):
            for x in range(SUB):
                at = (d * groups + f) * SUB + x
                moved = w_ref[at]
                out[pl.ds((d * groups + f) * SUB * SUB + x, SUB, stride=SUB), :] = (
                    moved * (1.0 + g_ref[at]) * r_ref[x, f])
        return 0

    lax.fori_loop(0, dirs, write, 0)
    lax.fori_loop(1, n, finish, 0)
    per_tile = 128 // SUB
    block = lax.broadcasted_iota(jnp.int32, (band, 128), 1) // SUB
    for tile in range(max(1, n // per_tile)):
        for c in range(4):
            built = jnp.zeros((band, 128), jnp.float32)
            for k in range(min(n, per_tile)):
                moved = pltpu.roll(recv[tile * per_tile + k], (SUB * (k - c)) % 128, 1)
                built = jnp.where(block == k, moved, built)
            ocean[c, :, tile * 128:(tile + 1) * 128] = built


def per_device(n, spectrum, wind, land_sea, band_rows):
    dirs, freqs, columns, lats = spectrum.shape
    groups = freqs // SUB
    half = dirs // 2 * groups
    band = lats // n
    f32 = jnp.float32
    vmem = pl.BlockSpec(memory_space=pltpu.VMEM)
    anywhere = pl.BlockSpec(memory_space=pltpu.HBM)
    cells = dirs * groups * SUB
    after, ocean = pl.pallas_call(
        functools.partial(kernel, n, dirs, groups),
        out_shape=(jax.ShapeDtypeStruct((cells * SUB, lats), f32),
                   jax.ShapeDtypeStruct((4, band, columns * n), f32)),
        in_specs=[anywhere] * 4,
        out_specs=(vmem, vmem),
        scratch_shapes=[
            pltpu.SMEM((2, dirs), f32),
            pltpu.VMEM((4, groups, SUB, lats), f32),
            pltpu.VMEM((2, SUB, lats), f32),
            pltpu.VMEM((SUB, lats), jnp.int32),
            pltpu.VMEM((1, lats), jnp.int32),
            pltpu.VMEM((cells * SUB, lats), f32),
            pltpu.VMEM((cells, SUB, lats), f32),
            pltpu.VMEM((cells, SUB, lats), f32),
            pltpu.VMEM((3, half, SUB, lats), f32),
            pltpu.VMEM((3, half, SUB, lats), f32),
            pltpu.VMEM((3, half, SUB, lats), f32),
            pltpu.VMEM((3, half, SUB, lats), f32),
            pltpu.VMEM((2, 2, SUB, lats), f32),
            pltpu.VMEM((2, SUB, lats), jnp.int32),
            pltpu.VMEM((2, 12, SUB, lats), f32),
            pltpu.VMEM((12, SUB, lats), f32),
            pltpu.VMEM((16, groups, SUB, lats), f32),
            pltpu.VMEM((SUB, groups, SUB, lats), f32),
            pltpu.VMEM((2, SUB, lats), f32),
            pltpu.VMEM((2, 2, SUB, lats), f32),
            pltpu.VMEM((128, 128), f32),
            pltpu.VMEM((n, band, 128), f32),
            pltpu.VMEM((n, band, 128), f32),
            pltpu.SemaphoreType.DMA((4,)),
            pltpu.SemaphoreType.DMA((3,)),
            pltpu.SemaphoreType.DMA((14,)),
            pltpu.SemaphoreType.DMA((14,)),
            pltpu.SemaphoreType.DMA((n,)),
            pltpu.SemaphoreType.DMA((n,)),
        ],
        compiler_params=pltpu.CompilerParams(
            collective_id=0, has_side_effects=True, vmem_limit_bytes=48 * 2**20),
        name="wave_window",
    )(spectrum.reshape(cells * SUB, lats), wind, land_sea,
      band_rows.reshape(1, lats))
    return after.reshape(spectrum.shape), ocean


def solution(mesh):
    placed = (
        P(None, None, ("member", "gx"), None),
        P(None, ("member", "gx"), None),
        P("gx", None),
        P(),
    )
    return jax.shard_map(
        functools.partial(per_device, mesh.shape["gx"]),
        mesh=mesh,
        in_specs=placed,
        out_specs=(P(None, None, ("member", "gx"), None), P(None, "gx", "member")),
        check_vma=False,
    )
```

```python
import functools
import math

import jax
import jax.numpy as jnp
from jax import lax
from jax.experimental import pallas as pl
from jax.experimental.pallas import tpu as pltpu
from jax.sharding import PartitionSpec as P

STEPS = 3
SUB = 8
LEFT, RIGHT = 8, 10


def kernel(n, dirs, groups, spec, wind_in, land_in, bands_in, out, ocean,
           trig, freq, wind, land, bands, x_ref, w_ref, g_ref, send_e, send_w, halo_l, halo_r, wind_h, land_h,
           wind_b, mask_b, r_ref, acc, e_send, e_halo, rows, sends, recv,
           in_sem, small_sem, ssem, rsem, a_ssem, a_rsem):
    me = lax.axis_index("gx")
    right, left = lax.rem(me + 1, n), lax.rem(me + n - 1, n)
    quarter = dirs // 4
    qrows = quarter * groups * SUB * SUB
    cells = dirs * groups * SUB
    lane = lax.broadcasted_iota(jnp.int32, (SUB, 128), 1)
    quads = [(q * quarter, q in (0, 3), q in (0, 1)) for q in range(4)]

    def in_copy(q):
        part = pl.ds(q * qrows, qrows)
        return pltpu.make_async_copy(spec.at[part], x_ref.at[part], in_sem.at[q])

    tables_in = [pltpu.make_async_copy(src, dst, small_sem.at[i]) for i, (src, dst) in enumerate(
        [(wind_in, wind), (land_in, land), (bands_in, bands)])]
    for copy in tables_in:
        copy.start()
    for q in range(4):
        in_copy(q).start()

    for d in range(dirs):
        angle = (d + 0.5) * (2.0 * math.pi / dirs)
        trig[0, d] = jnp.float32(math.cos(angle))
        trig[1, d] = jnp.float32(math.sin(angle))
    freqs = groups * SUB
    for f in range(groups):
        level = (lax.broadcasted_iota(jnp.int32, (SUB, 128), 0) + f * SUB).astype(jnp.float32)
        weight = (level + 1.0) * (1.0 / freqs)
        grown = jnp.exp(level * math.log(1.1))
        freq[0, f] = 0.45 / grown
        freq[1, f] = grown * (2.0 * math.pi * 0.0418 / 9.81)
        freq[2, f] = 0.3 * weight * weight
        freq[3, f] = weight * (3.0 / math.sqrt(dirs * freqs))

    barrier = pltpu.get_barrier_semaphore()

    def greet(i, _):
        pl.semaphore_signal(barrier, inc=1, device_id={"gx": lax.rem(me + i, n)},
                            device_id_type=pl.DeviceIdType.MESH)
        return 0

    lax.fori_loop(1, n, greet, 0)

    def remote(src, dst, slot, target):
        return pltpu.make_async_remote_copy(
            src_ref=src, dst_ref=dst, send_sem=ssem.at[slot], recv_sem=rsem.at[slot],
            device_id={"gx": target}, device_id_type=pl.DeviceIdType.MESH)

    bulk_e = [remote(send_e.at[k], halo_l.at[k], k, right) for k in range(3)]
    bulk_w = [remote(send_w.at[k], halo_r.at[k], 3 + k, left) for k in range(3)]
    small = [remote(wind, wind_h.at[0], 6, right), remote(wind, wind_h.at[1], 7, left),
             remote(land, land_h.at[0], 8, right), remote(land, land_h.at[1], 9, left)]
    energy_msg = [[remote(e_send.at[s], e_halo.at[s, 0], 10 + 2 * s, right),
                   remote(e_send.at[s], e_halo.at[s, 1], 11 + 2 * s, left)] for s in range(2)]

    for q, (d0, east, north) in enumerate(quads):
        in_copy(q).wait()
        base = d0 * groups
        local = (0 if q in (0, 1) else quarter) * groups

        def pack(i, _, base=base, local=local, east=east):
            for k in range(3):
                column = SUB - 1 - k if east else k
                value = x_ref[pl.ds((base + i) * SUB * SUB + column, SUB, stride=SUB), :]
                (send_e if east else send_w)[k, local + i] = value
            return 0

        lax.fori_loop(0, quarter * groups, pack, 0, unroll=4)

    for copy in tables_in:
        copy.wait()

    def spread(slot, wind_tile, land_tile, column):
        for c in range(2):
            wind_b[c, slot] = jnp.broadcast_to(wind_tile[c][column:column + 1], (SUB, 128))
        mask_b[slot] = jnp.broadcast_to(
            land_tile[column:column + 1].astype(jnp.float32), (SUB, 128))

    own_wind = [wind[0], wind[1]]
    own_land = land[...]
    for x in range(SUB):
        spread(x, own_wind, own_land, x)

    pl.semaphore_wait(barrier, n - 1)
    for copy in small + [bulk_e[0], bulk_w[0], bulk_e[1], bulk_w[1]]:
        copy.start()

    def scalars(d):
        return trig[0, d], trig[1, d]

    halves = [(0, 2 * quarter, True), (quarter, 0, False)]

    def coefficients(cosine, sine, f, east, turn):
        k = freq[0, f]
        along_x = k * (cosine if east else -cosine)
        along_y = k * jnp.abs(sine)
        centre = 1.0 - along_x - along_y
        return centre, along_x, jnp.where(lane == 127 * turn, 0.0, along_y)

    def shifted(value, turn):
        return pltpu.roll(value, 1 + 126 * turn, 1)

    def growth_of(cosine, sine, f, slot):
        ratio = (wind_b[0, slot] * cosine + wind_b[1, slot] * sine) * freq[1, f]
        return 0.05 * jnp.minimum(jnp.maximum(ratio - 1.0, 0.0), 4.0)

    zero = jnp.zeros((SUB, 128), jnp.float32)

    def main(step, sums):
        for d0, skip, east in halves:
            def body(i, sums, d0=d0, skip=skip, east=east):
                turn = i // quarter
                d = d0 + i + skip * turn
                cosine, sine = scalars(d)
                sums = list(sums)
                if step == 0:
                    speed = [wind_b[0, x] * cosine + wind_b[1, x] * sine for x in range(SUB)]
                for f in range(groups):
                    centre, along_x, along_y = coefficients(cosine, sine, f, east, turn)
                    before = None
                    for x in (range(SUB) if east else range(SUB - 1, -1, -1)):
                        at = (d * groups + f) * SUB + x
                        if step == 0:
                            value = x_ref[pl.ds((d * groups + f) * SUB * SUB + x, SUB, stride=SUB), :]
                            g_ref[at] = 0.05 * jnp.minimum(
                                jnp.maximum(speed[x] * freq[1, f] - 1.0, 0.0), 4.0)
                        else:
                            value = w_ref[at] * (1.0 + g_ref[at]) * r_ref[x, f]
                        new = centre * value + along_y * shifted(value, turn)
                        if before is not None:
                            new = new + along_x * before
                        before = value
                        w_ref[at] = new
                        sums[x] = sums[x] + new
                return tuple(sums)

            sums = lax.fori_loop(0, 2 * quarter, body, tuple(sums))
        return sums

    def fix(step, sums):
        first, last = sums[0], sums[SUB - 1]
        for d0, skip, east in halves:
            halo = halo_l if east else halo_r
            slot = LEFT if east else RIGHT
            edge = 0 if east else SUB - 1

            def body(i, total, d0=d0, skip=skip, east=east, halo=halo, slot=slot, edge=edge):
                turn = i // quarter
                d = d0 + i + skip * turn
                cosine, sine = scalars(d)
                for f in range(groups):
                    centre, along_x, along_y = coefficients(cosine, sine, f, east, turn)
                    at = i * groups + f

                    def advance(value, upwind, depth, s):
                        moved = centre * value + along_x * upwind + along_y * shifted(value, turn)
                        growth = growth_of(cosine, sine, f, slot + depth)
                        return moved * (1.0 + growth) * r_ref[slot + depth + 4 * (s if depth == 0 else 0), f]

                    if step == 0:
                        flow = halo[0, at]
                    elif step == 1:
                        flow = advance(halo[0, at], halo[1, at], 0, 0)
                        halo[0, at] = flow
                    else:
                        far = advance(halo[1, at], halo[2, at], 1, 0)
                        flow = advance(halo[0, at], far, 0, 1)
                    extra = along_x * flow
                    cell = (d * groups + f) * SUB + edge
                    w_ref[cell] = w_ref[cell] + extra
                    total = total + extra
                    if step == STEPS - 1:
                        flux = g_ref[cell] * extra
                        for c, part in enumerate((flux, flux, extra + flux, extra + flux)):
                            acc[c, edge, f] = acc[c, edge, f] + (sine if c % 2 else cosine) * part
                return total

            if east:
                first = lax.fori_loop(0, 2 * quarter, body, first)
            else:
                last = lax.fori_loop(0, 2 * quarter, body, last)
        return (first,) + tuple(sums[1:-1]) + (last,)

    def gather():
        for f in range(groups):
            def body(d, carry, f=f):
                cosine, sine = scalars(d)
                carry = list(carry)
                for x in range(SUB):
                    at = (d * groups + f) * SUB + x
                    moved = w_ref[at]
                    flux = g_ref[at] * moved
                    after = moved + flux
                    for c, part in enumerate((flux, flux, after, after)):
                        carry[c * SUB + x] = carry[c * SUB + x] + (sine if c % 2 else cosine) * part
                return tuple(carry)

            carry = lax.fori_loop(0, dirs, body, (zero,) * (4 * SUB))
            for c in range(4):
                for x in range(SUB):
                    acc[c, x, f] = carry[c * SUB + x]

    def energy_tile(sums):
        return jnp.concatenate(
            [jnp.sum(s * mask_b[x], axis=0, keepdims=True) for x, s in enumerate(sums)],
            axis=0) * (1.0 / cells)

    def factor(tile, column, mask_slot, slot):
        ratio = jnp.broadcast_to(tile[column:column + 1], (SUB, 128))
        for f in range(groups):
            r_ref[slot, f] = mask_b[mask_slot] / (1.0 + freq[2, f] * ratio)

    def own_factors(tile):
        ratio = tile / (0.5 + tile)
        for x in range(SUB):
            factor(ratio, x, x, x)

    sums = main(0, (zero,) * SUB)
    for copy in small:
        copy.wait()
    for side in range(2):
        tiles = [wind_h[side, 0], wind_h[side, 1]]
        land_tile = land_h[side]
        for depth in range(2):
            spread((LEFT if side == 0 else RIGHT) + depth, tiles, land_tile,
                   SUB - 1 - depth if side == 0 else depth)
    bulk_e[0].wait()
    bulk_w[0].wait()
    sums = fix(0, sums)
    for step in (1, 2):
        tile = energy_tile(sums)
        e_send[step - 1] = tile
        own_factors(tile)
        for copy in energy_msg[step - 1]:
            copy.start()
        if step == 1:
            bulk_e[2].start()
            bulk_w[2].start()
        sums = main(step, (zero,) * SUB)
        if step == STEPS - 1:
            gather()
        bulk_e[step].wait()
        bulk_w[step].wait()
        for copy in energy_msg[step - 1]:
            copy.wait()
        for side in range(2):
            seen = e_halo[step - 1, side]
            ratio = seen / (0.5 + seen)
            base = LEFT if side == 0 else RIGHT
            for depth in range(3 - step):
                factor(ratio, SUB - 1 - depth if side == 0 else depth, base + depth,
                       base + depth + 4 * (step - 1))
        sums = fix(step, sums)

    own_factors(energy_tile(sums))

    total = []
    for c in range(4):
        for x in range(SUB):
            value = zero
            for f in range(groups):
                scale = mask_b[x] if c < 2 else r_ref[x, f]
                value = value + acc[c, x, f] * (freq[3, f] * scale)
            total.append(jnp.sum(value, axis=0, keepdims=True))
    total.append(jnp.zeros((128 - 4 * SUB, 128), jnp.float32))
    stacked = jnp.concatenate(total, axis=0)
    lat = lax.broadcasted_iota(jnp.int32, (128, 128), 0)
    pick = (lat == bands[...]).astype(jnp.float32)
    picked = jnp.dot(stacked, pick, precision=lax.Precision.HIGHEST,
                     preferred_element_type=jnp.float32)
    rows[...] = picked.T
    band = 128 // n
    for k in range(n):
        sends[k] = rows[pl.ds(k * band, band), :]

    def exchange(i):
        target = lax.rem(me + i, n)
        return pltpu.make_async_remote_copy(
            src_ref=sends.at[target], dst_ref=recv.at[me], send_sem=a_ssem.at[i],
            recv_sem=a_rsem.at[i], device_id={"gx": target},
            device_id_type=pl.DeviceIdType.MESH)

    def begin(i, _):
        exchange(i).start()
        return 0

    def finish(i, _):
        exchange(i).wait()
        return 0

    lax.fori_loop(1, n, begin, 0)
    recv[pl.ds(me, 1)] = sends[pl.ds(me, 1)]

    def write(d, _):
        for f in range(groups):
            for x in range(SUB):
                at = (d * groups + f) * SUB + x
                moved = w_ref[at]
                out[pl.ds((d * groups + f) * SUB * SUB + x, SUB, stride=SUB), :] = (
                    moved * (1.0 + g_ref[at]) * r_ref[x, f])
        return 0

    lax.fori_loop(0, dirs, write, 0)
    lax.fori_loop(1, n, finish, 0)
    per_tile = 128 // SUB
    block = lax.broadcasted_iota(jnp.int32, (band, 128), 1) // SUB
    for tile in range(max(1, n // per_tile)):
        for c in range(4):
            built = jnp.zeros((band, 128), jnp.float32)
            for k in range(min(n, per_tile)):
                moved = pltpu.roll(recv[tile * per_tile + k], (SUB * (k - c)) % 128, 1)
                built = jnp.where(block == k, moved, built)
            ocean[c, :, tile * 128:(tile + 1) * 128] = built


def per_device(n, spectrum, wind, land_sea, band_rows):
    dirs, freqs, columns, lats = spectrum.shape
    groups = freqs // SUB
    half = dirs // 2 * groups
    band = lats // n
    f32 = jnp.float32
    vmem = pl.BlockSpec(memory_space=pltpu.VMEM)
    anywhere = pl.BlockSpec(memory_space=pltpu.HBM)
    cells = dirs * groups * SUB
    after, ocean = pl.pallas_call(
        functools.partial(kernel, n, dirs, groups),
        out_shape=(jax.ShapeDtypeStruct((cells * SUB, lats), f32),
                   jax.ShapeDtypeStruct((4, band, columns * n), f32)),
        in_specs=[anywhere] * 4,
        out_specs=(vmem, vmem),
        scratch_shapes=[
            pltpu.SMEM((2, dirs), f32),
            pltpu.VMEM((4, groups, SUB, lats), f32),
            pltpu.VMEM((2, SUB, lats), f32),
            pltpu.VMEM((SUB, lats), jnp.int32),
            pltpu.VMEM((1, lats), jnp.int32),
            pltpu.VMEM((cells * SUB, lats), f32),
            pltpu.VMEM((cells, SUB, lats), f32),
            pltpu.VMEM((cells, SUB, lats), f32),
            pltpu.VMEM((3, half, SUB, lats), f32),
            pltpu.VMEM((3, half, SUB, lats), f32),
            pltpu.VMEM((3, half, SUB, lats), f32),
            pltpu.VMEM((3, half, SUB, lats), f32),
            pltpu.VMEM((2, 2, SUB, lats), f32),
            pltpu.VMEM((2, SUB, lats), jnp.int32),
            pltpu.VMEM((2, 12, SUB, lats), f32),
            pltpu.VMEM((12, SUB, lats), f32),
            pltpu.VMEM((16, groups, SUB, lats), f32),
            pltpu.VMEM((4, SUB, groups, SUB, lats), f32),
            pltpu.VMEM((2, SUB, lats), f32),
            pltpu.VMEM((2, 2, SUB, lats), f32),
            pltpu.VMEM((128, 128), f32),
            pltpu.VMEM((n, band, 128), f32),
            pltpu.VMEM((n, band, 128), f32),
            pltpu.SemaphoreType.DMA((4,)),
            pltpu.SemaphoreType.DMA((3,)),
            pltpu.SemaphoreType.DMA((14,)),
            pltpu.SemaphoreType.DMA((14,)),
            pltpu.SemaphoreType.DMA((n,)),
            pltpu.SemaphoreType.DMA((n,)),
        ],
        compiler_params=pltpu.CompilerParams(
            collective_id=0, has_side_effects=True, vmem_limit_bytes=48 * 2**20),
        name="wave_window",
    )(spectrum.reshape(cells * SUB, lats), wind, land_sea,
      band_rows.reshape(1, lats))
    return after.reshape(spectrum.shape), ocean


def solution(mesh):
    placed = (
        P(None, None, ("member", "gx"), None),
        P(None, ("member", "gx"), None),
        P("gx", None),
        P(),
    )
    return jax.shard_map(
        functools.partial(per_device, mesh.shape["gx"]),
        mesh=mesh,
        in_specs=placed,
        out_specs=(P(None, None, ("member", "gx"), None), P(None, "gx", "member")),
        check_vma=False,
    )
```

```python
import functools
import math

import jax
import jax.numpy as jnp
from jax import lax
from jax.experimental import pallas as pl
from jax.experimental.pallas import tpu as pltpu
from jax.sharding import PartitionSpec as P

STEPS = 3
SUB = 8
LEFT, RIGHT = 8, 10


def kernel(n, dirs, groups, spec, wind_in, land_in, bands_in, out, ocean,
           trig, freq, wind, land, bands, x_ref, w_ref, g_ref, send_e, send_w, halo_l, halo_r, wind_h, land_h,
           wind_b, mask_b, r_ref, drift_ref, e_send, e_halo, rows, sends, recv,
           in_sem, small_sem, ssem, rsem, a_ssem, a_rsem):
    me = lax.axis_index("gx")
    right, left = lax.rem(me + 1, n), lax.rem(me + n - 1, n)
    quarter = dirs // 4
    qrows = quarter * groups * SUB * SUB
    cells = dirs * groups * SUB
    lane = lax.broadcasted_iota(jnp.int32, (SUB, 128), 1)
    quads = [(q * quarter, q in (0, 3), q in (0, 1)) for q in range(4)]

    def in_copy(q):
        part = pl.ds(q * qrows, qrows)
        return pltpu.make_async_copy(spec.at[part], x_ref.at[part], in_sem.at[q])

    tables_in = [pltpu.make_async_copy(src, dst, small_sem.at[i]) for i, (src, dst) in enumerate(
        [(wind_in, wind), (land_in, land), (bands_in, bands)])]
    for copy in tables_in:
        copy.start()
    for q in range(4):
        in_copy(q).start()

    for d in range(dirs):
        angle = (d + 0.5) * (2.0 * math.pi / dirs)
        trig[0, d] = jnp.float32(math.cos(angle))
        trig[1, d] = jnp.float32(math.sin(angle))
    freqs = groups * SUB
    for f in range(groups):
        level = (lax.broadcasted_iota(jnp.int32, (SUB, 128), 0) + f * SUB).astype(jnp.float32)
        weight = (level + 1.0) * (1.0 / freqs)
        grown = jnp.exp(level * math.log(1.1))
        freq[0, f] = 0.45 / grown
        freq[1, f] = grown * (2.0 * math.pi * 0.0418 / 9.81)
        freq[2, f] = 0.3 * weight * weight
        freq[3, f] = weight * (3.0 / math.sqrt(dirs * freqs))

    barrier = pltpu.get_barrier_semaphore()

    def greet(i, _):
        pl.semaphore_signal(barrier, inc=1, device_id={"gx": lax.rem(me + i, n)},
                            device_id_type=pl.DeviceIdType.MESH)
        return 0

    lax.fori_loop(1, n, greet, 0)

    def remote(src, dst, slot, target):
        return pltpu.make_async_remote_copy(
            src_ref=src, dst_ref=dst, send_sem=ssem.at[slot], recv_sem=rsem.at[slot],
            device_id={"gx": target}, device_id_type=pl.DeviceIdType.MESH)

    bulk_e = [remote(send_e.at[k], halo_l.at[k], k, right) for k in range(3)]
    bulk_w = [remote(send_w.at[k], halo_r.at[k], 3 + k, left) for k in range(3)]
    small = [remote(wind, wind_h.at[0], 6, right), remote(wind, wind_h.at[1], 7, left),
             remote(land, land_h.at[0], 8, right), remote(land, land_h.at[1], 9, left)]
    energy_msg = [[remote(e_send.at[s], e_halo.at[s, 0], 10 + 2 * s, right),
                   remote(e_send.at[s], e_halo.at[s, 1], 11 + 2 * s, left)] for s in range(2)]

    for q, (d0, east, north) in enumerate(quads):
        in_copy(q).wait()
        base = d0 * groups
        local = (0 if q in (0, 1) else quarter) * groups

        def pack(i, _, base=base, local=local, east=east):
            for k in range(3):
                column = SUB - 1 - k if east else k
                value = x_ref[pl.ds((base + i) * SUB * SUB + column, SUB, stride=SUB), :]
                (send_e if east else send_w)[k, local + i] = value
            return 0

        lax.fori_loop(0, quarter * groups, pack, 0, unroll=4)

    for copy in tables_in:
        copy.wait()

    def spread(slot, wind_tile, land_tile, column):
        for c in range(2):
            wind_b[c, slot] = jnp.broadcast_to(wind_tile[c][column:column + 1], (SUB, 128))
        mask_b[slot] = jnp.broadcast_to(
            land_tile[column:column + 1].astype(jnp.float32), (SUB, 128))

    own_wind = [wind[0], wind[1]]
    own_land = land[...]
    for x in range(SUB):
        spread(x, own_wind, own_land, x)

    pl.semaphore_wait(barrier, n - 1)
    for copy in small + [bulk_e[0], bulk_w[0], bulk_e[1], bulk_w[1]]:
        copy.start()

    def scalars(d):
        return trig[0, d], trig[1, d]

    halves = [(0, 2 * quarter, True), (quarter, 0, False)]

    def coefficients(cosine, sine, f, east, turn):
        k = freq[0, f]
        along_x = k * (cosine if east else -cosine)
        along_y = k * jnp.abs(sine)
        centre = 1.0 - along_x - along_y
        return centre, along_x, jnp.where(lane == 127 * turn, 0.0, along_y)

    def shifted(value, turn):
        return pltpu.roll(value, 1 + 126 * turn, 1)

    def growth_of(cosine, sine, f, slot):
        ratio = (wind_b[0, slot] * cosine + wind_b[1, slot] * sine) * freq[1, f]
        return 0.05 * jnp.minimum(jnp.maximum(ratio - 1.0, 0.0), 4.0)

    zero = jnp.zeros((SUB, 128), jnp.float32)

    def main(step, sums):
        for d0, skip, east in halves:
            def body(i, sums, d0=d0, skip=skip, east=east):
                turn = i // quarter
                d = d0 + i + skip * turn
                cosine, sine = scalars(d)
                sums = list(sums)
                if step == 0:
                    speed = [wind_b[0, x] * cosine + wind_b[1, x] * sine for x in range(SUB)]
                for f in range(groups):
                    centre, along_x, along_y = coefficients(cosine, sine, f, east, turn)
                    before = None
                    for x in (range(SUB) if east else range(SUB - 1, -1, -1)):
                        at = (d * groups + f) * SUB + x
                        if step == 0:
                            value = x_ref[pl.ds((d * groups + f) * SUB * SUB + x, SUB, stride=SUB), :]
                            g_ref[at] = 0.05 * jnp.minimum(
                                jnp.maximum(speed[x] * freq[1, f] - 1.0, 0.0), 4.0)
                        else:
                            value = w_ref[at] * (1.0 + g_ref[at]) * r_ref[x, f]
                        new = centre * value + along_y * shifted(value, turn)
                        if before is not None:
                            new = new + along_x * before
                        before = value
                        w_ref[at] = new
                        sums[x] = sums[x] + new
                return tuple(sums)

            sums = lax.fori_loop(0, 2 * quarter, body, tuple(sums), unroll=2)
        return sums

    def fix(step, sums):
        first, last = sums[0], sums[SUB - 1]
        for d0, skip, east in halves:
            halo = halo_l if east else halo_r
            slot = LEFT if east else RIGHT
            edge = 0 if east else SUB - 1

            def body(i, total, d0=d0, skip=skip, east=east, halo=halo, slot=slot, edge=edge):
                turn = i // quarter
                d = d0 + i + skip * turn
                cosine, sine = scalars(d)
                for f in range(groups):
                    centre, along_x, along_y = coefficients(cosine, sine, f, east, turn)
                    at = i * groups + f

                    def advance(value, upwind, depth, s):
                        moved = centre * value + along_x * upwind + along_y * shifted(value, turn)
                        growth = growth_of(cosine, sine, f, slot + depth)
                        return moved * (1.0 + growth) * r_ref[slot + depth + 4 * (s if depth == 0 else 0), f]

                    if step == 0:
                        flow = halo[0, at]
                    elif step == 1:
                        flow = advance(halo[0, at], halo[1, at], 0, 0)
                        halo[0, at] = flow
                    else:
                        far = advance(halo[1, at], halo[2, at], 1, 0)
                        flow = advance(halo[0, at], far, 0, 1)
                    extra = along_x * flow
                    cell = (d * groups + f) * SUB + edge
                    w_ref[cell] = w_ref[cell] + extra
                    total = total + extra
                return total

            if east:
                first = lax.fori_loop(0, 2 * quarter, body, first, unroll=3)
            else:
                last = lax.fori_loop(0, 2 * quarter, body, last, unroll=3)
        return (first,) + tuple(sums[1:-1]) + (last,)

    def energy_tile(sums):
        return jnp.concatenate(
            [jnp.sum(s * mask_b[x], axis=0, keepdims=True) for x, s in enumerate(sums)],
            axis=0) * (1.0 / cells)

    def factor(tile, column, mask_slot, slot):
        ratio = jnp.broadcast_to(tile[column:column + 1], (SUB, 128))
        for f in range(groups):
            r_ref[slot, f] = mask_b[mask_slot] / (1.0 + freq[2, f] * ratio)

    def own_factors(tile):
        ratio = tile / (0.5 + tile)
        for x in range(SUB):
            factor(ratio, x, x, x)

    sums = main(0, (zero,) * SUB)
    for copy in small:
        copy.wait()
    for side in range(2):
        tiles = [wind_h[side, 0], wind_h[side, 1]]
        land_tile = land_h[side]
        for depth in range(2):
            spread((LEFT if side == 0 else RIGHT) + depth, tiles, land_tile,
                   SUB - 1 - depth if side == 0 else depth)
    bulk_e[0].wait()
    bulk_w[0].wait()
    sums = fix(0, sums)
    for step in (1, 2):
        tile = energy_tile(sums)
        e_send[step - 1] = tile
        own_factors(tile)
        for copy in energy_msg[step - 1]:
            copy.start()
        if step == 1:
            bulk_e[2].start()
            bulk_w[2].start()
        sums = main(step, (zero,) * SUB)
        bulk_e[step].wait()
        bulk_w[step].wait()
        for copy in energy_msg[step - 1]:
            copy.wait()
        for side in range(2):
            seen = e_halo[step - 1, side]
            ratio = seen / (0.5 + seen)
            base = LEFT if side == 0 else RIGHT
            for depth in range(3 - step):
                factor(ratio, SUB - 1 - depth if side == 0 else depth, base + depth,
                       base + depth + 4 * (step - 1))
        sums = fix(step, sums)

    own_factors(energy_tile(sums))

    def gather(d, carry):
        cosine, sine = scalars(d)
        carry = list(carry)
        for x in range(SUB):
            flux, drift = zero, zero
            for f in range(groups):
                at = (d * groups + f) * SUB + x
                moved = w_ref[at]
                flow = g_ref[at] * moved
                flux = flux + freq[3, f] * flow
                drift = drift + drift_ref[x, f] * (moved + flow)
            carry[x] = carry[x] + cosine * flux
            carry[SUB + x] = carry[SUB + x] + sine * flux
            carry[2 * SUB + x] = carry[2 * SUB + x] + cosine * drift
            carry[3 * SUB + x] = carry[3 * SUB + x] + sine * drift
        return tuple(carry)

    for x in range(SUB):
        for f in range(groups):
            drift_ref[x, f] = freq[3, f] * r_ref[x, f]
    carry = lax.fori_loop(0, dirs, gather, (zero,) * (4 * SUB), unroll=2)

    total = []
    for j, value in enumerate(carry):
        if j < 2 * SUB:
            value = value * mask_b[j % SUB]
        total.append(jnp.sum(value, axis=0, keepdims=True))
    total.append(jnp.zeros((128 - 4 * SUB, 128), jnp.float32))
    stacked = jnp.concatenate(total, axis=0)
    lat = lax.broadcasted_iota(jnp.int32, (128, 128), 0)
    pick = (lat == bands[...]).astype(jnp.float32)
    picked = jnp.dot(stacked, pick, precision=lax.Precision.HIGHEST,
                     preferred_element_type=jnp.float32)
    rows[...] = picked.T
    band = 128 // n
    for k in range(n):
        sends[k] = rows[pl.ds(k * band, band), :]

    def exchange(i):
        target = lax.rem(me + i, n)
        return pltpu.make_async_remote_copy(
            src_ref=sends.at[target], dst_ref=recv.at[me], send_sem=a_ssem.at[i],
            recv_sem=a_rsem.at[i], device_id={"gx": target},
            device_id_type=pl.DeviceIdType.MESH)

    def begin(i, _):
        exchange(i).start()
        return 0

    def finish(i, _):
        exchange(i).wait()
        return 0

    lax.fori_loop(1, n, begin, 0)
    recv[pl.ds(me, 1)] = sends[pl.ds(me, 1)]

    def write(d, _):
        for f in range(groups):
            for x in range(SUB):
                at = (d * groups + f) * SUB + x
                moved = w_ref[at]
                out[pl.ds((d * groups + f) * SUB * SUB + x, SUB, stride=SUB), :] = (
                    moved * (1.0 + g_ref[at]) * r_ref[x, f])
        return 0

    lax.fori_loop(0, dirs, write, 0, unroll=2)
    lax.fori_loop(1, n, finish, 0)
    per_tile = 128 // SUB
    block = lax.broadcasted_iota(jnp.int32, (band, 128), 1) // SUB
    for tile in range(max(1, n // per_tile)):
        for c in range(4):
            built = jnp.zeros((band, 128), jnp.float32)
            for k in range(min(n, per_tile)):
                moved = pltpu.roll(recv[tile * per_tile + k], (SUB * (k - c)) % 128, 1)
                built = jnp.where(block == k, moved, built)
            ocean[c, :, tile * 128:(tile + 1) * 128] = built


def per_device(n, spectrum, wind, land_sea, band_rows):
    dirs, freqs, columns, lats = spectrum.shape
    groups = freqs // SUB
    half = dirs // 2 * groups
    band = lats // n
    f32 = jnp.float32
    vmem = pl.BlockSpec(memory_space=pltpu.VMEM)
    anywhere = pl.BlockSpec(memory_space=pltpu.HBM)
    cells = dirs * groups * SUB
    after, ocean = pl.pallas_call(
        functools.partial(kernel, n, dirs, groups),
        out_shape=(jax.ShapeDtypeStruct((cells * SUB, lats), f32),
                   jax.ShapeDtypeStruct((4, band, columns * n), f32)),
        in_specs=[anywhere] * 4,
        out_specs=(vmem, vmem),
        scratch_shapes=[
            pltpu.SMEM((2, dirs), f32),
            pltpu.VMEM((4, groups, SUB, lats), f32),
            pltpu.VMEM((2, SUB, lats), f32),
            pltpu.VMEM((SUB, lats), jnp.int32),
            pltpu.VMEM((1, lats), jnp.int32),
            pltpu.VMEM((cells * SUB, lats), f32),
            pltpu.VMEM((cells, SUB, lats), f32),
            pltpu.VMEM((cells, SUB, lats), f32),
            pltpu.VMEM((3, half, SUB, lats), f32),
            pltpu.VMEM((3, half, SUB, lats), f32),
            pltpu.VMEM((3, half, SUB, lats), f32),
            pltpu.VMEM((3, half, SUB, lats), f32),
            pltpu.VMEM((2, 2, SUB, lats), f32),
            pltpu.VMEM((2, SUB, lats), jnp.int32),
            pltpu.VMEM((2, 12, SUB, lats), f32),
            pltpu.VMEM((12, SUB, lats), f32),
            pltpu.VMEM((16, groups, SUB, lats), f32),
            pltpu.VMEM((SUB, groups, SUB, lats), f32),
            pltpu.VMEM((2, SUB, lats), f32),
            pltpu.VMEM((2, 2, SUB, lats), f32),
            pltpu.VMEM((128, 128), f32),
            pltpu.VMEM((n, band, 128), f32),
            pltpu.VMEM((n, band, 128), f32),
            pltpu.SemaphoreType.DMA((4,)),
            pltpu.SemaphoreType.DMA((3,)),
            pltpu.SemaphoreType.DMA((14,)),
            pltpu.SemaphoreType.DMA((14,)),
            pltpu.SemaphoreType.DMA((n,)),
            pltpu.SemaphoreType.DMA((n,)),
        ],
        compiler_params=pltpu.CompilerParams(
            collective_id=0, has_side_effects=True, vmem_limit_bytes=48 * 2**20),
        name="wave_window",
    )(spectrum.reshape(cells * SUB, lats), wind, land_sea,
      band_rows.reshape(1, lats))
    return after.reshape(spectrum.shape), ocean


def solution(mesh):
    placed = (
        P(None, None, ("member", "gx"), None),
        P(None, ("member", "gx"), None),
        P("gx", None),
        P(),
    )
    return jax.shard_map(
        functools.partial(per_device, mesh.shape["gx"]),
        mesh=mesh,
        in_specs=placed,
        out_specs=(P(None, None, ("member", "gx"), None), P(None, "gx", "member")),
        check_vma=False,
    )
```
